512 devices in a mesh: lag: 4 (over x_hi, core), row: 32 (over z, x_lo), col: 4 (over y).
Axes of the slice: x: 4 (x_hi: 2, x_lo: 2; x = x_hi * 2 + x_lo), y: 4, z: 16, core: 2. Of those that a mesh axis runs over, the one named last changes fastest.
Arguments:
- impedance: bfloat16 [4, 12288, 12288], P('lag', 'row', 'col'), may hold values from -0.013671875 to 0.013671875
- history: bfloat16 [4, 4, 32, 96, 128], P('lag', 'col', 'row'), may hold values from -6 to 6
- excitation: float32 [2, 32, 16, 24, 128], P(None, 'row', ('lag', 'col')), may hold values from -6 to 6
- inv_self: float32 [12288], P('row'), may hold values from 0.4 to 1.2
- cubic_coef: float32 [12288], P('row'), may hold values from 0.01 to 0.1
Outputs:
- currents: float32 [2, 32, 16, 24, 128], P(None, 'row', ('lag', 'col'))
The draws below stay inside these ranges and needn't reach their ends.
All inputs are finite; a program needn't handle non-finite values.
Results may differ from the reference program's by a relative error of at most 0.00054.
Values may be sent and summed in bfloat16 or wider, within the bound.
No kernel may reach another device: no remote copies, remote signals or barrier semaphores. Data moves between devices by JAX's collectives and lax.ppermute only.
A program may use at most 64 MiB of HBM per device.

```python
import math
import jax
import jax.numpy as jnp

N = 12288
LAGS = 4
STEPS = 2
E = 128
SHARE = 24
PIECE = 96
N_LAG = 4
N_ROW = 32
N_COL = 4


def level_of(own_key, shape, cuts, smallest, top_value):
    level, own = 1.0, jax.random.fold_in(own_key, 6)
    for dim, blocks in cuts:
        heights = jnp.exp(jax.random.uniform(jax.random.fold_in(own, dim), (blocks,), jnp.float32, smallest / len(cuts), top_value / len(cuts)))
        level = level * jnp.repeat(heights, shape[dim] // blocks).reshape([-1 if axis == dim else 1 for axis in range(len(shape))])
    return level


def gaussian(stream_key, shape, scale, bound, pieces=(), held_as=jnp.bfloat16):
    gain = level_of(stream_key, shape, pieces, -0.22, 0.18) if pieces else 1.0
    entries = jax.random.normal(stream_key, shape, jnp.float32) * scale * gain
    return jnp.minimum(jnp.maximum(entries, -bound), bound).astype(held_as)


def setup_inputs(seed: int = 0) -> dict:
    key_list = jax.random.split(jax.random.key(seed), 6)
    impedance = gaussian(key_list[0], (LAGS, N, N), (16 * N) ** -0.5, 0.013671875, ((0, 4), (1, 32), (2, 4)))
    history = gaussian(key_list[1], (LAGS, N_COL, N_ROW, PIECE, E), 1.0, 6.0, ((0, 4), (1, 4), (2, 32)))
    excitation = gaussian(key_list[2], (STEPS, N_ROW, N_LAG * N_COL, SHARE, E), 1.0, 6.0, ((1, 32), (2, 16)), jnp.float32)
    inv_self = jnp.clip(jnp.exp(math.log(1.2) - 1.0986123 * jax.random.uniform(key_list[3], (N,), jnp.float32) ** level_of(key_list[3], (N,), ((0, 32),), -0.2, 0.2)), 0.4, 1.2)
    cubic_coef = jnp.clip(jnp.exp(math.log(0.1) - 2.3025851 * jax.random.uniform(key_list[4], (N,), jnp.float32) ** level_of(key_list[4], (N,), ((0, 32),), -0.2, 0.2)), 0.01, 0.1)
    return dict(impedance=impedance, history=history, excitation=excitation, inv_self=inv_self, cubic_coef=cubic_coef)


def reference(impedance, history, excitation, inv_self, cubic_coef):
    width = excitation.shape[-1]
    drive = excitation.reshape(STEPS, N, width)
    past = history.reshape(LAGS, N, width)
    fresh_list = []
    results = []
    for moment in range(STEPS):
        residual = drive[moment]
        for lagged in range(LAGS):
            if moment - lagged - 1 >= 0:
                source = fresh_list[moment - lagged - 1]
            else:
                source = past[lagged - moment]
            residual = residual - jnp.dot(impedance[lagged], source, preferred_element_type=jnp.float32)
        scaled = residual * inv_self[:, None]
        current = scaled + cubic_coef[:, None] * scaled * scaled * scaled
        results.append(current)
        fresh_list.append(current.astype(jnp.bfloat16))
    return jnp.stack(results).reshape(excitation.shape)
```

```python
import jax
import jax.numpy as jnp
from jax import lax
from jax.sharding import Mesh
from jax.sharding import PartitionSpec as P

STEPS = 2
LAG = ("x_hi", "core")
Z = ("z_hi", "z_lo")
ROW = ("z_hi", "z_lo", "x_lo")
LC = ("x_hi", "core", "y")


def exchange(x, axes):
    return lax.all_to_all(x, axes, split_axis=0, concat_axis=0, tiled=True)


def to_all(x, axes):
    return exchange(jnp.broadcast_to(x, (lax.axis_size(axes), *x.shape)), axes)


def update(residual, inv_rows, coef_rows):
    scaled = residual * inv_rows[:, None]
    return scaled + coef_rows[:, None] * scaled * scaled * scaled


def shards(impedance, history, excitation, inv_self, cubic_coef):
    lag = lax.axis_index(LAG)
    share = lax.axis_index(LC)
    share_rows, width = excitation.shape[3:]
    matrix = impedance[0]
    rows, cols = matrix.shape
    offset = share * share_rows
    inv_rows = lax.dynamic_slice_in_dim(inv_self, offset, share_rows, 0)
    coef_rows = lax.dynamic_slice_in_dim(cubic_coef, offset, share_rows, 0)

    piece = history[0, 0, 0]
    by_z = to_all(piece, Z)
    both = lax.all_gather(by_z, "x_lo", axis=1)
    stored = both.reshape(cols, width)

    def owned(source, moment):
        product = jnp.dot(matrix, source, preferred_element_type=jnp.float32)
        shares = product.reshape(-1, share_rows, width)
        total = exchange(shares, LC).sum(axis=0)
        return update(excitation[moment, 0, 0] - total, inv_rows, coef_rows)

    first = owned(stored, 0)
    shifted = lax.ppermute(stored, LAG, [(k, k + 1) for k in range(3)])
    fresh = to_all(first.astype(jnp.bfloat16), Z)
    n_hi, n_lo, n_x = (lax.axis_size(a) for a in ("z_hi", "z_lo", "x_lo"))
    fresh = fresh.reshape(n_hi, n_lo, share_rows, width)
    n_xhi, n_core, n_y = (lax.axis_size(a) for a in LC)
    planes = jnp.broadcast_to(fresh, (n_xhi, n_x, *fresh.shape))
    planes = planes.reshape(-1, n_lo, share_rows, width)
    planes = exchange(planes, ("x_hi", "x_lo", "y"))
    planes = lax.all_gather(planes, "core")
    planes = planes.reshape(n_core, n_xhi, n_x, n_y, n_lo, share_rows, width)
    block = planes.transpose(4, 2, 1, 0, 3, 5, 6).reshape(cols, width)
    second = owned(jnp.where(lag == 0, block, shifted), 1)
    return jnp.stack([first, second])[:, None, None]


def solution(mesh):
    split = Mesh(
        mesh.devices.reshape(2, 2, 4, 4, 2, 4),
        ("x_hi", "core", "z_hi", "z_lo", "x_lo", "y"),
    )
    in_specs = (
        P(LAG, ROW, "y"),
        P(LAG, "y", ROW, None, None),
        P(None, ROW, LC, None, None),
        P(ROW),
        P(ROW),
    )
    out_specs = P(None, ROW, LC, None, None)
    return jax.shard_map(
        shards, mesh=split, in_specs=in_specs, out_specs=out_specs, check_vma=False
    )
```

```python
import jax
import jax.numpy as jnp
from jax import lax
from jax.sharding import Mesh
from jax.sharding import PartitionSpec as P

STEPS = 2
LAG = ("x_hi", "core")
Z = ("z_hi", "z_lo")
ROW = ("z_hi", "z_lo", "x_lo")
LC = ("x_hi", "core", "y")


def exchange(x, axes):
    return lax.all_to_all(x, axes, split_axis=0, concat_axis=0, tiled=True)


def to_all(x, axes):
    return exchange(jnp.broadcast_to(x, (lax.axis_size(axes), *x.shape)), axes)


def update(residual, inv_rows, coef_rows):
    scaled = residual * inv_rows[:, None]
    return scaled + coef_rows[:, None] * scaled * scaled * scaled


def shards(impedance, history, excitation, inv_self, cubic_coef):
    lag = lax.axis_index(LAG)
    share = lax.axis_index(LC)
    share_rows, width = excitation.shape[3:]
    matrix = impedance[0]
    rows, cols = matrix.shape
    offset = share * share_rows
    inv_rows = lax.dynamic_slice_in_dim(inv_self, offset, share_rows, 0)
    coef_rows = lax.dynamic_slice_in_dim(cubic_coef, offset, share_rows, 0)

    piece = history[0, 0, 0]
    pair = lax.all_gather(piece, "x_lo")
    stored = lax.all_gather(pair, Z).reshape(cols, width)

    def owned(source, moment):
        product = jnp.dot(matrix, source, preferred_element_type=jnp.float32)
        shares = product.reshape(-1, share_rows, width)
        total = exchange(shares, LC).sum(axis=0)
        return update(excitation[moment, 0, 0] - total, inv_rows, coef_rows)

    first = owned(stored, 0)
    shifted = lax.ppermute(stored, LAG, [(k, k + 1) for k in range(3)])
    fresh = to_all(first.astype(jnp.bfloat16), Z)
    n_hi, n_lo, n_x = (lax.axis_size(a) for a in ("z_hi", "z_lo", "x_lo"))
    fresh = fresh.reshape(n_hi, n_lo, share_rows, width)
    n_xhi, n_core, n_y = (lax.axis_size(a) for a in LC)
    planes = jnp.broadcast_to(fresh, (n_xhi, n_x, *fresh.shape))
    planes = planes.reshape(-1, n_lo, share_rows, width)
    planes = exchange(planes, ("x_hi", "x_lo", "y"))
    planes = lax.all_gather(planes, "core")
    planes = planes.reshape(n_core, n_xhi, n_x, n_y, n_lo, share_rows, width)
    block = planes.transpose(4, 2, 1, 0, 3, 5, 6).reshape(cols, width)
    second = owned(jnp.where(lag == 0, block, shifted), 1)
    return jnp.stack([first, second])[:, None, None]


def solution(mesh):
    split = Mesh(
        mesh.devices.reshape(2, 2, 4, 4, 2, 4),
        ("x_hi", "core", "z_hi", "z_lo", "x_lo", "y"),
    )
    in_specs = (
        P(LAG, ROW, "y"),
        P(LAG, "y", ROW, None, None),
        P(None, ROW, LC, None, None),
        P(ROW),
        P(ROW),
    )
    out_specs = P(None, ROW, LC, None, None)
    return jax.shard_map(
        shards, mesh=split, in_specs=in_specs, out_specs=out_specs, check_vma=False
    )
```

```python
import jax
import jax.numpy as jnp
from jax import lax
from jax.experimental import pallas as pl
from jax.experimental.pallas import tpu as pltpu
from jax.experimental.layout import Layout, with_layout_constraint
from jax.sharding import Mesh
from jax.sharding import PartitionSpec as P

LAG = ("x_hi", "core")
Z = ("z_hi", "z_lo")
ROW = ("z_hi", "z_lo", "x_lo")
LC = ("x_hi", "core", "y")
XLC = ("x_lo", "x_hi", "core", "y")


def exchange(x, axes):
    return lax.all_to_all(x, axes, split_axis=0, concat_axis=0, tiled=True)


def to_all(x, axes):
    return exchange(jnp.broadcast_to(x, (lax.axis_size(axes), *x.shape)), axes)


def update(residual, inv_rows, coef_rows):
    scaled = residual * inv_rows[:, None]
    return scaled + coef_rows[:, None] * scaled * scaled * scaled


def turn_kernel(m_ref, o_ref):
    n_x, count, n_z, size, _ = o_ref.shape
    span = count * size
    for j in range(n_x * n_z):
        turned = m_ref[:, j * span : (j + 1) * span].T
        for k in range(count):
            o_ref[j % n_x, k, j // n_x] = turned[k * size : (k + 1) * size]


def turn(matrix, n_x, count, size):
    rows, cols = matrix.shape
    shape = (n_x, count, cols // (n_x * count * size), size, rows)
    return pl.pallas_call(
        turn_kernel,
        in_specs=[pl.BlockSpec(memory_space=pltpu.VMEM)],
        out_specs=pl.BlockSpec(memory_space=pltpu.VMEM),
        out_shape=jax.ShapeDtypeStruct(shape, matrix.dtype),
    )(matrix)


def row_major(x):
    return with_layout_constraint(x, Layout(major_to_minor=tuple(range(x.ndim))))


def shards(impedance, history, excitation, inv_self, cubic_coef):
    share = lax.axis_index(LC)
    share_rows, width = excitation.shape[3:]
    matrix = impedance[0]
    rows, cols = matrix.shape
    offset = share * share_rows
    inv_rows = lax.dynamic_slice_in_dim(inv_self, offset, share_rows, 0)
    coef_rows = lax.dynamic_slice_in_dim(cubic_coef, offset, share_rows, 0)
    n_x, n_y, n_share = (lax.axis_size(a) for a in ("x_lo", "y", LC))

    piece = history[0, 0, 0]
    other = lax.ppermute(piece, "x_lo", [(0, 1), (1, 0)])
    slices = turn(matrix, n_x, n_share, share_rows)
    slices = slices.reshape(n_x * n_share, -1, rows)
    even = lax.axis_index("x_lo") == 0
    pair = jnp.stack([jnp.where(even, piece, other), jnp.where(even, other, piece)])
    slices = exchange(slices, XLC)
    slices = slices.reshape(n_x, n_share, -1, rows)[:, :n_y].reshape(n_x, -1, rows)
    stored = lax.all_gather(pair, Z).reshape(cols, width)

    def owned(shares, axes, moment):
        total = exchange(shares, axes)
        return update(excitation[moment, 0, 0] - total.sum(axis=0), inv_rows, coef_rows)

    shifted = lax.ppermute(stored, LAG, [(k, k + 1) for k in range(3)])
    older = jnp.dot(matrix, shifted, preferred_element_type=jnp.float32)
    older = row_major(lax.optimization_barrier(row_major(older)))
    product = row_major(jnp.dot(matrix, stored, preferred_element_type=jnp.float32))
    first = owned(product.reshape(-1, share_rows, width), LC, 0)
    fresh = to_all(first.astype(jnp.bfloat16), Z).reshape(-1, width)
    newer = jnp.stack(
        [
            lax.dot_general(
                slices[k],
                fresh,
                (((0,), (0,)), ((), ())),
                preferred_element_type=jnp.float32,
            )
            + jnp.where(lax.axis_index("x_lo") == k, older, 0.0)
            for k in range(n_x)
        ]
    )
    second = owned(row_major(newer).reshape(-1, share_rows, width), XLC, 1)
    return jnp.stack([first, second])[:, None, None]


def solution(mesh):
    split = Mesh(
        mesh.devices.reshape(2, 2, 4, 4, 2, 4),
        ("x_hi", "core", "z_hi", "z_lo", "x_lo", "y"),
    )
    in_specs = (
        P(LAG, ROW, "y"),
        P(LAG, "y", ROW, None, None),
        P(None, ROW, LC, None, None),
        P(ROW),
        P(ROW),
    )
    out_specs = P(None, ROW, LC, None, None)
    return jax.shard_map(
        shards, mesh=split, in_specs=in_specs, out_specs=out_specs, check_vma=False
    )
```

```python
import jax
import jax.numpy as jnp
from jax import lax
from jax.experimental import pallas as pl
from jax.experimental.pallas import tpu as pltpu
from jax.experimental.layout import Layout, with_layout_constraint
from jax.sharding import Mesh
from jax.sharding import PartitionSpec as P

LAG = ("x_hi", "core")
Z = ("z_hi", "z_lo")
ROW = ("z_hi", "z_lo", "x_lo")
LC = ("x_hi", "core", "y")
XLC = ("x_lo", "x_hi", "core", "y")


def exchange(x, axes):
    return lax.all_to_all(x, axes, split_axis=0, concat_axis=0, tiled=True)


def to_all(x, axes):
    return exchange(jnp.broadcast_to(x, (lax.axis_size(axes), *x.shape)), axes)


def update(residual, inv_rows, coef_rows):
    scaled = residual * inv_rows[:, None]
    return scaled + coef_rows[:, None] * scaled * scaled * scaled


def turn_kernel(m_hbm, o_hbm, m_buf, o_buf, in_sem, out_sem):
    n_x, count, n_z, size, _ = o_buf.shape
    span = count * size
    part = n_x * span

    def read(z):
        return pltpu.make_async_copy(
            m_hbm.at[:, z * part : (z + 1) * part], m_buf.at[z], in_sem.at[z]
        )

    def write(z):
        return pltpu.make_async_copy(
            o_buf.at[:, :, z], o_hbm.at[:, :, z], out_sem.at[z]
        )

    for z in range(n_z):
        read(z).start()
    for z in range(n_z):
        read(z).wait()
        for x in range(n_x):
            turned = m_buf[z, :, x * span : (x + 1) * span].T
            for k in range(count):
                o_buf[x, k, z] = turned[k * size : (k + 1) * size]
        write(z).start()
    for z in range(n_z):
        write(z).wait()


def turn(matrix, n_x, count, size):
    rows, cols = matrix.shape
    n_z = cols // (n_x * count * size)
    shape = (n_x, count, n_z, size, rows)
    return pl.pallas_call(
        turn_kernel,
        in_specs=[pl.BlockSpec(memory_space=pl.ANY)],
        out_specs=pl.BlockSpec(memory_space=pl.ANY),
        out_shape=jax.ShapeDtypeStruct(shape, matrix.dtype),
        scratch_shapes=[
            pltpu.VMEM((n_z, rows, cols // n_z), matrix.dtype),
            pltpu.VMEM(shape, matrix.dtype),
            pltpu.SemaphoreType.DMA((n_z,)),
            pltpu.SemaphoreType.DMA((n_z,)),
        ],
    )(matrix)


def row_major(x):
    return with_layout_constraint(x, Layout(major_to_minor=tuple(range(x.ndim))))


def shards(impedance, history, excitation, inv_self, cubic_coef):
    share = lax.axis_index(LC)
    share_rows, width = excitation.shape[3:]
    matrix = impedance[0]
    rows, cols = matrix.shape
    offset = share * share_rows
    inv_rows = lax.dynamic_slice_in_dim(inv_self, offset, share_rows, 0)
    coef_rows = lax.dynamic_slice_in_dim(cubic_coef, offset, share_rows, 0)
    n_x, n_y, n_share = (lax.axis_size(a) for a in ("x_lo", "y", LC))

    piece = history[0, 0, 0]
    other = lax.ppermute(piece, "x_lo", [(0, 1), (1, 0)])
    slices = turn(matrix, n_x, n_share, share_rows)
    slices = slices.reshape(n_x * n_share, -1, rows)
    even = lax.axis_index("x_lo") == 0
    pair = jnp.stack([jnp.where(even, piece, other), jnp.where(even, other, piece)])
    slices = exchange(slices, XLC)
    slices = slices.reshape(n_x, n_share, -1, rows)[:, :n_y].reshape(n_x, -1, rows)
    stored = lax.all_gather(pair, Z).reshape(cols, width)

    def owned(shares, axes, moment):
        total = exchange(shares, axes)
        return update(excitation[moment, 0, 0] - total.sum(axis=0), inv_rows, coef_rows)

    shifted = lax.ppermute(stored, LAG, [(k, k + 1) for k in range(3)])
    older = jnp.dot(matrix, shifted, preferred_element_type=jnp.float32)
    older = row_major(lax.optimization_barrier(row_major(older)))
    product = row_major(jnp.dot(matrix, stored, preferred_element_type=jnp.float32))
    first = owned(product.reshape(-1, share_rows, width), LC, 0)
    fresh = to_all(first.astype(jnp.bfloat16), Z).reshape(-1, width)
    newer = lax.dot_general(
        slices,
        jnp.broadcast_to(fresh, (n_x, *fresh.shape)),
        (((1,), (1,)), ((0,), (0,))),
        preferred_element_type=jnp.float32,
    )
    mine = lax.broadcasted_iota(jnp.int32, (n_x, 1, 1), 0) == lax.axis_index("x_lo")
    newer = newer + jnp.where(mine, older, 0.0)
    second = owned(row_major(newer).reshape(-1, share_rows, width), XLC, 1)
    return jnp.stack([first, second])[:, None, None]


def solution(mesh):
    split = Mesh(
        mesh.devices.reshape(2, 2, 4, 4, 2, 4),
        ("x_hi", "core", "z_hi", "z_lo", "x_lo", "y"),
    )
    in_specs = (
        P(LAG, ROW, "y"),
        P(LAG, "y", ROW, None, None),
        P(None, ROW, LC, None, None),
        P(ROW),
        P(ROW),
    )
    out_specs = P(None, ROW, LC, None, None)
    return jax.shard_map(
        shards, mesh=split, in_specs=in_specs, out_specs=out_specs, check_vma=False
    )
```

```python
import jax
import jax.numpy as jnp
from jax import lax
from jax.experimental import pallas as pl
from jax.experimental.pallas import tpu as pltpu
from jax.experimental.layout import Layout, with_layout_constraint
from jax.sharding import Mesh
from jax.sharding import PartitionSpec as P

LAG = ("x_hi", "core")
Z = ("z_hi", "z_lo")
ROW = ("z_hi", "z_lo", "x_lo")
LC = ("x_hi", "core", "y")
XLC = ("x_lo", "x_hi", "core", "y")


def exchange(x, axes):
    return lax.all_to_all(x, axes, split_axis=0, concat_axis=0, tiled=True)


def to_all(x, axes):
    return exchange(jnp.broadcast_to(x, (lax.axis_size(axes), *x.shape)), axes)


def update(residual, inv_rows, coef_rows):
    scaled = residual * inv_rows[:, None]
    return scaled + coef_rows[:, None] * scaled * scaled * scaled


def turn_kernel(m_hbm, o_hbm, m_buf, o_buf, in_sem, out_sem):
    n_x, count, n_z, size, _ = o_buf.shape
    span = count * size
    part = n_x * span

    def read(z):
        return pltpu.make_async_copy(
            m_hbm.at[:, z * part : (z + 1) * part], m_buf.at[z], in_sem.at[z]
        )

    def write(z):
        return pltpu.make_async_copy(
            o_buf.at[:, :, z], o_hbm.at[:, :, z], out_sem.at[z]
        )

    @pl.when(lax.axis_index(LAG) == 0)
    def _():
        for z in range(n_z):
            read(z).start()
        for z in range(n_z):
            read(z).wait()
            for x in range(n_x):
                turned = m_buf[z, :, x * span : (x + 1) * span].T
                for k in range(count):
                    o_buf[x, k, z] = turned[k * size : (k + 1) * size]
            write(z).start()
        for z in range(n_z):
            write(z).wait()


def turn(matrix, n_x, count, size):
    rows, cols = matrix.shape
    n_z = cols // (n_x * count * size)
    shape = (n_x, count, n_z, size, rows)
    return pl.pallas_call(
        turn_kernel,
        in_specs=[pl.BlockSpec(memory_space=pl.ANY)],
        out_specs=pl.BlockSpec(memory_space=pl.ANY),
        out_shape=jax.ShapeDtypeStruct(shape, matrix.dtype),
        scratch_shapes=[
            pltpu.VMEM((n_z, rows, cols // n_z), matrix.dtype),
            pltpu.VMEM(shape, matrix.dtype),
            pltpu.SemaphoreType.DMA((n_z,)),
            pltpu.SemaphoreType.DMA((n_z,)),
        ],
    )(matrix)


def row_major(x):
    return with_layout_constraint(x, Layout(major_to_minor=tuple(range(x.ndim))))


def shards(impedance, history, excitation, inv_self, cubic_coef):
    share = lax.axis_index(LC)
    share_rows, width = excitation.shape[3:]
    matrix = impedance[0]
    rows, cols = matrix.shape
    offset = share * share_rows
    inv_rows = lax.dynamic_slice_in_dim(inv_self, offset, share_rows, 0)
    coef_rows = lax.dynamic_slice_in_dim(cubic_coef, offset, share_rows, 0)
    n_x, n_y, n_share = (lax.axis_size(a) for a in ("x_lo", "y", LC))

    piece = history[0, 0, 0]
    other = lax.ppermute(piece, "x_lo", [(0, 1), (1, 0)])
    slices = turn(matrix, n_x, n_share, share_rows)
    slices = slices.reshape(n_x * n_share, -1, rows)
    even = lax.axis_index("x_lo") == 0
    low, high = jnp.where(even, piece, other), jnp.where(even, other, piece)
    pair = jnp.concatenate([low, high])
    slices = exchange(slices, XLC)
    slices = slices.reshape(n_x, n_share, -1, rows)[:, :n_y].reshape(n_x, -1, rows)
    stored = lax.all_gather(pair, Z).reshape(cols, width)

    def owned(shares, axes, moment):
        total = exchange(shares, axes)
        return update(excitation[moment, 0, 0] - total.sum(axis=0), inv_rows, coef_rows)

    shifted = lax.ppermute(stored, LAG, [(k, k + 1) for k in range(3)])
    older = jnp.dot(matrix, shifted, preferred_element_type=jnp.float32)
    older = row_major(lax.optimization_barrier(row_major(older)))
    product = row_major(jnp.dot(matrix, stored, preferred_element_type=jnp.float32))
    first = owned(product.reshape(-1, share_rows, width), LC, 0)
    fresh = to_all(first.astype(jnp.bfloat16), Z).reshape(-1, width)
    newer = lax.dot_general(
        slices,
        jnp.broadcast_to(fresh, (n_x, *fresh.shape)),
        (((1,), (1,)), ((0,), (0,))),
        preferred_element_type=jnp.float32,
    )
    mine = lax.broadcasted_iota(jnp.int32, (n_x, 1, 1), 0) == lax.axis_index("x_lo")
    newer = newer + jnp.where(mine, older, 0.0)
    second = owned(row_major(newer).reshape(-1, share_rows, width), XLC, 1)
    return jnp.stack([first, second])[:, None, None]


def solution(mesh):
    split = Mesh(
        mesh.devices.reshape(2, 2, 4, 4, 2, 4),
        ("x_hi", "core", "z_hi", "z_lo", "x_lo", "y"),
    )
    in_specs = (
        P(LAG, ROW, "y"),
        P(LAG, "y", ROW, None, None),
        P(None, ROW, LC, None, None),
        P(ROW),
        P(ROW),
    )
    out_specs = P(None, ROW, LC, None, None)
    return jax.shard_map(
        shards, mesh=split, in_specs=in_specs, out_specs=out_specs, check_vma=False
    )
```
